64 devices in a mesh: rep: 4 (over x, y), dp: 16 (over z, core).
Axes of the slice: x: 2, y: 2, z: 8, core: 2. Of those that a mesh axis runs over, the one named last changes fastest.
The devices are a block of a 4x4x8 slice.
Arguments:
- g_w_gate: bfloat16 [64, 2, 896, 2560], P(('rep', 'dp')), parts along dimension 0
- g_w_up: bfloat16 [64, 2, 896, 2560], P(('rep', 'dp')), parts along dimension 0
- g_w_down: bfloat16 [64, 2, 2560, 896], P(('rep', 'dp')), parts along dimension 0
- w_gate: bfloat16 [2, 896, 2560], replicated
- w_up: bfloat16 [2, 896, 2560], replicated
- w_down: bfloat16 [2, 2560, 896], replicated
- m_w_gate: float32 [2, 896, 2560], P(None, 'dp')
- m_w_up: float32 [2, 896, 2560], P(None, 'dp')
- m_w_down: float32 [2, 2560, 896], P(None, 'dp')
- v_w_gate: float32 [2, 896, 2560], P(None, 'dp')
- v_w_up: float32 [2, 896, 2560], P(None, 'dp')
- v_w_down: float32 [2, 2560, 896], P(None, 'dp')
Outputs:
- output 1: bfloat16 [8, 896, 2560], P('rep'), parts along dimension 0
- output 2: bfloat16 [8, 896, 2560], P('rep'), parts along dimension 0
- output 3: bfloat16 [8, 2560, 896], P('rep'), parts along dimension 0
- output 4: float32 [8, 896, 2560], P('rep', 'dp'), parts along dimension 0
- output 5: float32 [8, 896, 2560], P('rep', 'dp'), parts along dimension 0
- output 6: float32 [8, 2560, 896], P('rep', 'dp'), parts along dimension 0
- output 7: float32 [8, 896, 2560], P('rep', 'dp'), parts along dimension 0
- output 8: float32 [8, 896, 2560], P('rep', 'dp'), parts along dimension 0
- output 9: float32 [8, 2560, 896], P('rep', 'dp'), parts along dimension 0
There are 4 independent parts. The reference program is written for one: setup_inputs(seed, part) draws one part's arguments, and reference() takes and returns one part's arrays. A program takes and returns all parts, laid end to end along the dimension named above; an argument that names none is the same for every part.
All inputs are finite; a program needn't handle non-finite values.
Results may differ from the reference program's by a relative error of at most 0.022.
Values are sent between devices in bfloat16 or wider.
A program may use at most 768 MiB of HBM per device.

```python
import jax
import jax.numpy as jnp
from jax import lax

DEVICES = 16
D = 896
FF = 2560
LAYERS = 2
NAMES = ("w_gate", "w_up", "w_down")
SHAPES = {"w_gate": (LAYERS, D, FF), "w_up": (LAYERS, D, FF), "w_down": (LAYERS, FF, D)}


def setup_inputs(seed: int = 0, part: int = 0) -> dict:
    kz, *keys = jax.random.split(jax.random.key(seed), 1 + 5 * len(NAMES))
    loud = 2.0 ** jax.random.uniform(kz, (), jnp.float32, -1.0, 1.0)
    drawn = {}
    for name, key, both in zip(NAMES, keys[:3], keys[3:6], strict=True):
        own = jax.random.normal(jax.random.fold_in(key, part), (DEVICES, *SHAPES[name]), jnp.float32)
        shared = jax.random.normal(jax.random.fold_in(both, part), SHAPES[name], jnp.float32)
        drawn["g_" + name] = (loud * (0.7 * shared / DEVICES + 0.7 * own * DEVICES**-0.5)).astype(jnp.bfloat16)
    for name, key in zip(NAMES, keys[6:9], strict=True):
        drawn[name] = (jax.random.normal(key, SHAPES[name], jnp.float32) * SHAPES[name][1] ** -0.5).astype(jnp.bfloat16)
    for name, key in zip(NAMES, keys[9:12], strict=True):
        drawn["m_" + name] = loud * 0.5 * jax.random.normal(key, SHAPES[name], jnp.float32)
    for name, key in zip(NAMES, keys[12:15], strict=True):
        drawn["v_" + name] = loud * loud * jax.random.uniform(key, SHAPES[name], jnp.float32, 0.5, 1.5)
    return drawn


def adamw(w, m, v, g):
    m = 0.9 * m + 0.1 * g
    v = 0.95 * v + 0.05 * g * g
    step = m * lax.rsqrt(v + 1e-8) + 0.1 * w
    return (w - 0.02 * step).astype(jnp.bfloat16), m, v


def clipped(gradients, sum_of_squares, count):
    factor = jnp.minimum(1.0, 0.5 * lax.rsqrt(sum_of_squares / count + 1e-30))
    return [g * factor for g in gradients]


def reference(g_w_gate, g_w_up, g_w_down, w_gate, w_up, w_down, m_w_gate, m_w_up, m_w_down, v_w_gate, v_w_up, v_w_down):
    def total(terms):
        return lax.scan(lambda so_far, term: (so_far + term.astype(jnp.float32), None), jnp.zeros(terms.shape[1:], jnp.float32), terms)[0]

    gradients = [total(terms).astype(jnp.bfloat16).astype(jnp.float32) for terms in (g_w_gate, g_w_up, g_w_down)]
    gradients = clipped(gradients, sum(jnp.sum(g * g) for g in gradients), sum(g.size for g in gradients))
    new = [
        adamw(w.astype(jnp.float32), m, v, g)
        for w, m, v, g in zip((w_gate, w_up, w_down), (m_w_gate, m_w_up, m_w_down), (v_w_gate, v_w_up, v_w_down), gradients, strict=True)
    ]
    return tuple(one[which] for which in range(3) for one in new)
```

```python
import functools
import math

import jax
import jax.numpy as jnp
from jax import lax
from jax.experimental import pallas as pl
from jax.experimental.pallas import tpu as pltpu
from jax.sharding import PartitionSpec as P

MESH = pl.DeviceIdType.MESH
F32, BF16 = jnp.float32, jnp.bfloat16


def row_tile(rows, columns):
    best = 8
    for tile in range(8, rows + 1, 8):
        if rows % tile == 0 and tile * columns <= 32 * 1024:
            best = tile
    return best


def kernel(n, count, *refs):
    g, w, m_in, v_in = (refs[i : i + 3] for i in range(0, 12, 3))
    layers, chips = g[0].shape[0], n // 2
    new = [refs[12 + k * layers : 12 + (k + 1) * layers] for k in range(3)]
    refs = refs[12 + 3 * layers :]
    m, v, own, held = (refs[i : i + 3] for i in range(0, 12, 3))
    (squares, own_sem, pair_send, pair_recv, ring_send, ring_recv, gather_recv, hand_send, hand_recv, norm_send, norm_recv, moment_sem, old_sem) = refs[12:]
    pieces = [(k, l) for k in range(3) for l in range(layers)]
    number = {piece: i for i, piece in enumerate(pieces)}
    me = lax.axis_index("dp")
    h, z = lax.rem(me, 2), lax.div(me, 2)
    partner = me + 1 - 2 * h
    onward = [lax.rem(me + 2, n), lax.rem(me + n - 2, n)]

    def remote(src, dst, send, recv, device):
        return pltpu.make_async_remote_copy(
            src_ref=src, dst_ref=dst, send_sem=send, recv_sem=recv, device_id={"dp": device}, device_id_type=MESH
        )

    def chunk(l, stage):
        return lax.rem(z + 2 * chips - 1 - stage, chips) if l == 0 else lax.rem(z + 1 + stage, chips)

    def own_copy(k, l, stage, slot):
        c = chunk(l, stage)
        return pltpu.make_async_copy(g[k].at[l, 2 * c + h], own[k].at[l, c], own_sem.at[slot, number[k, l]])

    def pair_copy(k, l, stage, slot):
        c = chunk(l, stage)
        i = number[k, l]
        return remote(g[k].at[l, 2 * c + 1 - h], new[k][l].at[2 * c + h], pair_send.at[slot, i], pair_recv.at[stage, i], partner)

    def ring_copy(k, l, stage):
        c = chunk(l, stage)
        i = number[k, l]
        return remote(own[k].at[l, c], new[k][l].at[2 * c + h], ring_send.at[i], ring_recv.at[stage, i], onward[l])

    def source(l, step):
        return lax.rem(z + 2 * chips - 1 - step, chips) if l == 0 else lax.rem(z + 1 + step, chips)

    def gather_copy(k, l, c, step):
        rows = new[k][l].at[2 * c + h]
        i = number[k, l]
        return remote(rows, rows, ring_send.at[i], gather_recv.at[step, i], onward[l])

    def hand_copy(k, l, c, step):
        rows = new[k][l].at[2 * c + h]
        i = number[k, l]
        return remote(rows, rows, hand_send.at[i], hand_recv.at[step, i], partner)

    for k, l in pieces:
        own_copy(k, l, 0, 0).start()

    barrier = pltpu.get_barrier_semaphore()

    def greet(j, _):
        pl.semaphore_signal(barrier, inc=1, device_id={"dp": lax.rem(me + j, n)}, device_id_type=MESH)
        return 0

    lax.fori_loop(1, n, greet, 0)
    pl.semaphore_wait(barrier, n - 1)

    for stage in range(2):
        for k, l in pieces:
            pair_copy(k, l, stage, stage).start()
            if stage:
                own_copy(k, l, stage, stage).start()

    def add(k, l, stage, arrived, total=0, squared=False):
        c = chunk(l, stage)
        rows, columns = own[k].shape[2:]
        tile = row_tile(rows, columns)

        def body(i, total):
            at = pl.ds(pl.multiple_of(i * tile, tile), tile)
            x = own[k][l, c, at, :].astype(F32) + new[k][l][2 * c + 1 - h, at, :].astype(F32)
            if arrived:
                x = x + new[k][l][2 * c + h, at, :].astype(F32)
            x = x.astype(BF16)
            own[k][l, c, at, :] = x
            if not squared:
                return total
            y = x.astype(F32)
            y = y * y
            y = sum(y[:, j : j + 128] for j in range(0, columns, 128))
            return total + sum(y[j : j + 8] for j in range(0, tile, 8))

        return lax.fori_loop(0, rows // tile, body, total)

    for k, l in pieces:
        own_copy(k, l, 0, 0).wait()
        pair_copy(k, l, 0, 0).wait_recv()
        add(k, l, 0, False)
        ring_copy(k, l, 0).start()
    for k, l in pieces:
        own_copy(k, l, 2, 0).start()
        pair_copy(k, l, 0, 0).wait_send()
        pair_copy(k, l, 2, 0).start()

    def middle(stage, _):
        slot = lax.rem(stage, 2)
        for k, l in pieces:
            own_copy(k, l, stage, slot).wait()
            pair_copy(k, l, stage, slot).wait_recv()
            ring_copy(k, l, stage - 1).wait_recv()
            add(k, l, stage, True)
            ring_copy(k, l, stage - 1).wait_send()
            ring_copy(k, l, stage).start()

            @pl.when(stage + 2 < chips)
            def _():
                own_copy(k, l, stage + 2, slot).start()
                pair_copy(k, l, stage, slot).wait_send()
                pair_copy(k, l, stage + 2, slot).start()

        return 0

    lax.fori_loop(1, chips - 2, middle, 0)

    for k, l in pieces:
        i = number[k, l]
        pltpu.make_async_copy(m_in[k].at[l], m[k].at[l], moment_sem.at[0, i]).start()
        pltpu.make_async_copy(v_in[k].at[l], v[k].at[l], moment_sem.at[1, i]).start()
        pltpu.make_async_copy(w[k].at[l, me], held[k].at[l], old_sem.at[i]).start()

    lax.fori_loop(chips - 2, chips - 1, middle, 0)

    last = chips - 1
    total = jnp.zeros((8, 128), F32)
    for k, l in pieces:
        own_copy(k, l, last, last % 2).wait()
        pair_copy(k, l, last, last % 2).wait_recv()
        ring_copy(k, l, last - 1).wait_recv()
        total = add(k, l, last, True, total, True)

    squares[me] = jnp.sum(total, axis=0, keepdims=True)

    def tell(j):
        return remote(squares.at[me], squares.at[me], norm_send.at[j], norm_recv.at[j], lax.rem(me + j, n))

    def tell_start(j, _):
        tell(j).start()
        return 0

    def tell_wait(j, _):
        tell(j).wait()
        return 0

    lax.fori_loop(1, n, tell_start, 0)
    for k, l in pieces:
        i = number[k, l]
        pltpu.make_async_copy(m_in[k].at[l], m[k].at[l], moment_sem.at[0, i]).wait()
        pltpu.make_async_copy(v_in[k].at[l], v[k].at[l], moment_sem.at[1, i]).wait()
        pltpu.make_async_copy(w[k].at[l, me], held[k].at[l], old_sem.at[i]).wait()
        ring_copy(k, l, last - 1).wait_send()
        for stage in (last - 1, last):
            pair_copy(k, l, stage, stage % 2).wait_send()
    lax.fori_loop(1, n, tell_wait, 0)
    everything = jnp.sum(squares[...], axis=0)
    everything = jnp.sum(everything, axis=1, keepdims=True)
    factor = jnp.minimum(1.0, 0.5 * lax.rsqrt(everything / count + 1e-30))

    for k, l in pieces:
        rows, columns = held[k].shape[1:]
        tile = row_tile(rows, columns)

        def body(i, _):
            at = pl.ds(pl.multiple_of(i * tile, tile), tile)
            x = own[k][l, z, at, :].astype(F32) * factor
            m_new = 0.9 * m[k][l, at, :] + 0.1 * x
            v_new = 0.95 * v[k][l, at, :] + 0.05 * x * x
            old = held[k][l, at, :].astype(F32)
            m[k][l, at, :] = m_new
            v[k][l, at, :] = v_new
            new[k][l][me, at, :] = (old - 0.02 * (m_new * lax.rsqrt(v_new + 1e-8) + 0.1 * old)).astype(BF16)
            return 0

        lax.fori_loop(0, rows // tile, body, 0)
        gather_copy(k, l, z, 0).start()
        hand_copy(k, l, z, 0).start()

    def forward(step, _):
        for k, l in pieces:
            c = source(l, step)
            gather_copy(k, l, c, step).wait_recv()
            gather_copy(k, l, c, step).wait_send()
            gather_copy(k, l, c, step + 1).start()
            hand_copy(k, l, c, step).wait_send()
            hand_copy(k, l, c, step + 1).start()
        return 0

    lax.fori_loop(0, chips - 2, forward, 0)
    for k, l in pieces:
        step = chips - 2
        c = source(l, step)
        gather_copy(k, l, c, step).wait_recv()
        gather_copy(k, l, c, step).wait_send()
        hand_copy(k, l, c, step).wait_send()
        hand_copy(k, l, c, step + 1).start()

    def handed(step, _):
        for k, l in pieces:
            hand_copy(k, l, z, step).wait_recv()
        return 0

    lax.fori_loop(0, chips, handed, 0)
    for k, l in pieces:
        hand_copy(k, l, z, chips - 1).wait_send()


def put_out(layers, *refs):
    new, moments = refs[: 3 * layers], refs[3 * layers : 3 * layers + 6]
    outs, sem = refs[3 * layers + 6 : -1], refs[-1]
    pairs = [(one, outs[i // layers].at[i % layers]) for i, one in enumerate(new)] + list(zip(moments, outs[3:]))
    copies = [pltpu.make_async_copy(one, out, sem.at[i]) for i, (one, out) in enumerate(pairs)]
    for copy in copies:
        copy.start()
    for copy in copies:
        copy.wait()


def solution(mesh):
    n = mesh.shape["dp"]

    def step(*arrays):
        terms, weights, m, v = (arrays[i : i + 3] for i in (0, 3, 6, 9))
        layers = m[0].shape[0]
        parts = [one.shape[1:] for one in m]
        count = float(n * layers * sum(math.prod(part) for part in parts))
        cut = lambda a, part: a.reshape(layers, n, *part)
        terms = [cut(t, part) for t, part in zip(terms, parts)]
        weights = [cut(t, part) for t, part in zip(weights, parts)]
        chips, pieces = n // 2, 3 * layers
        sem = pltpu.SemaphoreType.DMA
        outs = [pltpu.VMEM((n, *part), BF16) for part in parts for _ in range(layers)] + [pltpu.VMEM((layers, *part), F32) for part in parts] * 2
        result = pl.pallas_call(
            functools.partial(kernel, n, count),
            out_shape=outs,
            in_specs=[pl.BlockSpec(memory_space=pltpu.HBM)] * 12,
            out_specs=[pl.BlockSpec(memory_space=pltpu.VMEM)] * len(outs),
            scratch_shapes=[pltpu.VMEM((layers, chips, *part), BF16) for part in parts]
            + [pltpu.VMEM((layers, *part), BF16) for part in parts]
            + [
                pltpu.VMEM((n, 1, 128), F32),
                sem((2, pieces)),
                sem((2, pieces)),
                sem((chips, pieces)),
                sem((pieces,)),
                sem((chips - 1, pieces)),
                sem((chips - 1, pieces)),
                sem((pieces,)),
                sem((chips, pieces)),
                sem((n,)),
                sem((n,)),
                sem((2, pieces)),
                sem((pieces,)),
            ],
            compiler_params=pltpu.CompilerParams(collective_id=0, has_side_effects=True, vmem_limit_bytes=24 * 1024 * 1024),
        )(*(pltpu.with_memory_space_constraint(one, pltpu.HBM) for one in (*terms, *weights, *m, *v)))
        result = [pltpu.with_memory_space_constraint(one, pltpu.VMEM) for one in result]
        result = pl.pallas_call(
            functools.partial(put_out, layers),
            out_shape=[pltpu.HBM((layers, n, *part), BF16) for part in parts] + [pltpu.HBM((layers, *part), F32) for part in parts] * 2,
            in_specs=[pl.BlockSpec(memory_space=pltpu.VMEM)] * len(result),
            out_specs=[pl.BlockSpec(memory_space=pltpu.HBM)] * 9,
            scratch_shapes=[sem((len(result),))],
            compiler_params=pltpu.CompilerParams(vmem_limit_bytes=1024 * 1024),
        )(*result)
        whole = [one.reshape(layers, -1, one.shape[-1]) for one in result[:3]]
        return (*whole, *result[3:])

    all_of, cut = P(None, None, None), P(None, "dp", None)
    return jax.shard_map(
        step,
        mesh=mesh,
        in_specs=(P(("rep", "dp"), None, None, None),) * 3 + (all_of,) * 3 + (cut,) * 6,
        out_specs=(P("rep", None, None),) * 3 + (P("rep", "dp", None),) * 6,
        check_vma=False,
    )
```

```python
import functools
import math

import jax
import jax.numpy as jnp
from jax import lax
from jax.experimental import pallas as pl
from jax.experimental.pallas import tpu as pltpu
from jax.sharding import PartitionSpec as P

MESH = pl.DeviceIdType.MESH
F32, BF16 = jnp.float32, jnp.bfloat16


def row_tile(rows, columns):
    best = 8
    for tile in range(8, rows + 1, 8):
        if rows % tile == 0 and tile * columns <= 32 * 1024:
            best = tile
    return best


def kernel(n, count, *refs):
    g, w, m_in, v_in = (refs[i : i + 3] for i in range(0, 12, 3))
    layers, chips = g[0].shape[0], n // 2
    new = [refs[12 + k * layers : 12 + (k + 1) * layers] for k in range(3)]
    refs = refs[12 + 3 * layers :]
    m, v, own, held = (refs[i : i + 3] for i in range(0, 12, 3))
    (squares, own_sem, pair_send, pair_recv, ring_send, ring_recv, gather_recv, hand_send, hand_recv, norm_send, norm_recv, moment_sem, old_sem) = refs[12:]
    pieces = [(k, l) for k in range(3) for l in range(layers)]
    number = {piece: i for i, piece in enumerate(pieces)}
    me = lax.axis_index("dp")
    h, z = lax.rem(me, 2), lax.div(me, 2)
    partner = me + 1 - 2 * h
    onward = [lax.rem(me + 2, n), lax.rem(me + n - 2, n)]

    def remote(src, dst, send, recv, device):
        return pltpu.make_async_remote_copy(
            src_ref=src, dst_ref=dst, send_sem=send, recv_sem=recv, device_id={"dp": device}, device_id_type=MESH
        )

    def chunk(l, stage):
        return lax.rem(z + 2 * chips - 1 - stage, chips) if l == 0 else lax.rem(z + 1 + stage, chips)

    def own_copy(k, l, stage, slot):
        c = chunk(l, stage)
        return pltpu.make_async_copy(g[k].at[l, 2 * c + h], own[k].at[l, c], own_sem.at[slot, number[k, l]])

    def pair_copy(k, l, stage, slot):
        c = chunk(l, stage)
        i = number[k, l]
        return remote(g[k].at[l, 2 * c + 1 - h], new[k][l].at[2 * c + h], pair_send.at[slot, i], pair_recv.at[stage, i], partner)

    def ring_copy(k, l, stage):
        c = chunk(l, stage)
        i = number[k, l]
        return remote(own[k].at[l, c], new[k][l].at[2 * c + h], ring_send.at[i], ring_recv.at[stage, i], onward[l])

    def source(l, step):
        return lax.rem(z + 2 * chips - 1 - step, chips) if l == 0 else lax.rem(z + 1 + step, chips)

    def gather_copy(k, l, c, step):
        rows = new[k][l].at[2 * c + h]
        i = number[k, l]
        return remote(rows, rows, ring_send.at[i], gather_recv.at[step, i], onward[l])

    def hand_copy(k, l, c, step):
        rows = new[k][l].at[2 * c + h]
        i = number[k, l]
        return remote(rows, rows, hand_send.at[i], hand_recv.at[step, i], partner)

    for k, l in pieces:
        own_copy(k, l, 0, 0).start()

    barrier = pltpu.get_barrier_semaphore()

    def greet(j, _):
        pl.semaphore_signal(barrier, inc=1, device_id={"dp": lax.rem(me + j, n)}, device_id_type=MESH)
        return 0

    lax.fori_loop(1, n, greet, 0)
    pl.semaphore_wait(barrier, n - 1)

    for stage in range(2):
        for k, l in pieces:
            pair_copy(k, l, stage, stage).start()
            if stage:
                own_copy(k, l, stage, stage).start()

    def add(k, l, stage, arrived, total=0, squared=False):
        c = chunk(l, stage)
        rows, columns = own[k].shape[2:]
        tile = row_tile(rows, columns)

        def body(i, total):
            at = pl.ds(pl.multiple_of(i * tile, tile), tile)
            x = own[k][l, c, at, :].astype(F32) + new[k][l][2 * c + 1 - h, at, :].astype(F32)
            if arrived:
                x = x + new[k][l][2 * c + h, at, :].astype(F32)
            x = x.astype(BF16)
            own[k][l, c, at, :] = x
            if not squared:
                return total
            y = x.astype(F32)
            y = y * y
            y = sum(y[:, j : j + 128] for j in range(0, columns, 128))
            return total + sum(y[j : j + 8] for j in range(0, tile, 8))

        return lax.fori_loop(0, rows // tile, body, total)

    for k, l in pieces:
        own_copy(k, l, 0, 0).wait()
        pair_copy(k, l, 0, 0).wait_recv()
        add(k, l, 0, False)
        ring_copy(k, l, 0).start()
    for k, l in pieces:
        own_copy(k, l, 2, 0).start()
        pair_copy(k, l, 0, 0).wait_send()
        pair_copy(k, l, 2, 0).start()

    def middle(stage, _):
        slot = lax.rem(stage, 2)
        for k, l in pieces:
            own_copy(k, l, stage, slot).wait()
            pair_copy(k, l, stage, slot).wait_recv()
            ring_copy(k, l, stage - 1).wait_recv()
            add(k, l, stage, True)
            ring_copy(k, l, stage - 1).wait_send()
            ring_copy(k, l, stage).start()

            @pl.when(stage + 2 < chips)
            def _():
                own_copy(k, l, stage + 2, slot).start()
                pair_copy(k, l, stage, slot).wait_send()
                pair_copy(k, l, stage + 2, slot).start()

        return 0

    lax.fori_loop(1, chips - 2, middle, 0)

    for k, l in pieces:
        i = number[k, l]
        pltpu.make_async_copy(m_in[k].at[l], m[k].at[l], moment_sem.at[0, i]).start()
        pltpu.make_async_copy(v_in[k].at[l], v[k].at[l], moment_sem.at[1, i]).start()
        pltpu.make_async_copy(w[k].at[l, me], held[k].at[l], old_sem.at[i]).start()

    lax.fori_loop(chips - 2, chips - 1, middle, 0)

    last = chips - 1
    total = jnp.zeros((8, 128), F32)
    for k, l in pieces:
        own_copy(k, l, last, last % 2).wait()
        pair_copy(k, l, last, last % 2).wait_recv()
        ring_copy(k, l, last - 1).wait_recv()
        total = add(k, l, last, True, total, True)

    squares[me] = jnp.sum(total, axis=0, keepdims=True)

    def tell(j):
        return remote(squares.at[me], squares.at[me], norm_send.at[j], norm_recv.at[j], lax.rem(me + j, n))

    def tell_start(j, _):
        tell(j).start()
        return 0

    def tell_wait(j, _):
        tell(j).wait()
        return 0

    lax.fori_loop(1, n, tell_start, 0)
    for k, l in pieces:
        i = number[k, l]
        pltpu.make_async_copy(m_in[k].at[l], m[k].at[l], moment_sem.at[0, i]).wait()
        pltpu.make_async_copy(v_in[k].at[l], v[k].at[l], moment_sem.at[1, i]).wait()
        pltpu.make_async_copy(w[k].at[l, me], held[k].at[l], old_sem.at[i]).wait()
        ring_copy(k, l, last - 1).wait_send()
        for stage in (last - 1, last):
            pair_copy(k, l, stage, stage % 2).wait_send()
    lax.fori_loop(1, n, tell_wait, 0)
    everything = jnp.sum(squares[...], axis=0)
    everything = jnp.sum(everything, axis=1, keepdims=True)
    factor = jnp.minimum(1.0, 0.5 * lax.rsqrt(everything / count + 1e-30))

    for k, l in pieces:
        rows, columns = held[k].shape[1:]
        tile = row_tile(rows, columns)

        def body(i, _):
            at = pl.ds(pl.multiple_of(i * tile, tile), tile)
            x = own[k][l, z, at, :].astype(F32) * factor
            m_new = 0.9 * m[k][l, at, :] + 0.1 * x
            v_new = 0.95 * v[k][l, at, :] + 0.05 * x * x
            old = held[k][l, at, :].astype(F32)
            m[k][l, at, :] = m_new
            v[k][l, at, :] = v_new
            new[k][l][me, at, :] = (old - 0.02 * (m_new * lax.rsqrt(v_new + 1e-8) + 0.1 * old)).astype(BF16)
            return 0

        lax.fori_loop(0, rows // tile, body, 0)
        gather_copy(k, l, z, 0).start()
        hand_copy(k, l, z, 0).start()

    def forward(step, _):
        for k, l in pieces:
            c = source(l, step)
            gather_copy(k, l, c, step).wait_recv()
            gather_copy(k, l, c, step).wait_send()
            gather_copy(k, l, c, step + 1).start()
            hand_copy(k, l, c, step).wait_send()
            hand_copy(k, l, c, step + 1).start()
        return 0

    lax.fori_loop(0, chips - 2, forward, 0)
    for k, l in pieces:
        step = chips - 2
        c = source(l, step)
        gather_copy(k, l, c, step).wait_recv()
        gather_copy(k, l, c, step).wait_send()
        hand_copy(k, l, c, step).wait_send()
        hand_copy(k, l, c, step + 1).start()

    def handed(step, _):
        for k, l in pieces:
            hand_copy(k, l, z, step).wait_recv()
        return 0

    lax.fori_loop(0, chips, handed, 0)
    for k, l in pieces:
        hand_copy(k, l, z, chips - 1).wait_send()


def put_out(layers, *refs):
    new, moments = refs[: 3 * layers], refs[3 * layers : 3 * layers + 6]
    outs, sem = refs[3 * layers + 6 : -1], refs[-1]
    pairs = [(one, outs[i // layers].at[i % layers]) for i, one in enumerate(new)] + list(zip(moments, outs[3:]))
    copies = [pltpu.make_async_copy(one, out, sem.at[i]) for i, (one, out) in enumerate(pairs)]
    for copy in copies:
        copy.start()
    for copy in copies:
        copy.wait()


def solution(mesh):
    n = mesh.shape["dp"]

    def step(*arrays):
        terms, weights, m, v = (arrays[i : i + 3] for i in (0, 3, 6, 9))
        layers = m[0].shape[0]
        parts = [one.shape[1:] for one in m]
        count = float(n * layers * sum(math.prod(part) for part in parts))
        cut = lambda a, part: a.reshape(layers, n, *part)
        terms = [cut(t, part) for t, part in zip(terms, parts)]
        weights = [cut(t, part) for t, part in zip(weights, parts)]
        chips, pieces = n // 2, 3 * layers
        sem = pltpu.SemaphoreType.DMA
        outs = [pltpu.VMEM((n, *part), BF16) for part in parts for _ in range(layers)] + [pltpu.VMEM((layers, *part), F32) for part in parts] * 2
        result = pl.pallas_call(
            functools.partial(kernel, n, count),
            out_shape=outs,
            in_specs=[pl.BlockSpec(memory_space=pltpu.HBM)] * 12,
            out_specs=[pl.BlockSpec(memory_space=pltpu.VMEM)] * len(outs),
            scratch_shapes=[pltpu.VMEM((layers, chips, *part), BF16) for part in parts]
            + [pltpu.VMEM((layers, *part), BF16) for part in parts]
            + [
                pltpu.VMEM((n, 1, 128), F32),
                sem((2, pieces)),
                sem((2, pieces)),
                sem((chips, pieces)),
                sem((pieces,)),
                sem((chips - 1, pieces)),
                sem((chips - 1, pieces)),
                sem((pieces,)),
                sem((chips, pieces)),
                sem((n,)),
                sem((n,)),
                sem((2, pieces)),
                sem((pieces,)),
            ],
            compiler_params=pltpu.CompilerParams(collective_id=0, has_side_effects=True, vmem_limit_bytes=24 * 1024 * 1024),
        )(*(pltpu.with_memory_space_constraint(one, pltpu.HBM) for one in (*terms, *weights, *m, *v)))
        result = [pltpu.with_memory_space_constraint(one, pltpu.VMEM) for one in result]
        result = pl.pallas_call(
            functools.partial(put_out, layers),
            out_shape=[pltpu.HBM((layers, n, *part), BF16) for part in parts] + [pltpu.HBM((layers, *part), F32) for part in parts] * 2,
            in_specs=[pl.BlockSpec(memory_space=pltpu.VMEM)] * len(result),
            out_specs=[pl.BlockSpec(memory_space=pltpu.HBM)] * 9,
            scratch_shapes=[sem((len(result),))],
            compiler_params=pltpu.CompilerParams(vmem_limit_bytes=24 * 1024 * 1024),
        )(*result)
        whole = [one.reshape(layers, -1, one.shape[-1]) for one in result[:3]]
        return (*whole, *result[3:])

    all_of, cut = P(None, None, None), P(None, "dp", None)
    return jax.shard_map(
        step,
        mesh=mesh,
        in_specs=(P(("rep", "dp"), None, None, None),) * 3 + (all_of,) * 3 + (cut,) * 6,
        out_specs=(P("rep", None, None),) * 3 + (P("rep", "dp", None),) * 6,
        check_vma=False,
    )
```

```python
import functools
import math

import jax
import jax.numpy as jnp
from jax import lax
from jax.experimental import pallas as pl
from jax.experimental.pallas import tpu as pltpu
from jax.sharding import PartitionSpec as P

MESH = pl.DeviceIdType.MESH
F32, BF16 = jnp.float32, jnp.bfloat16


def row_tile(rows, columns):
    best = 8
    for tile in range(8, rows + 1, 8):
        if rows % tile == 0 and tile * columns <= 32 * 1024:
            best = tile
    return best


def cuts(parts):
    *most, (rows, _) = parts
    small = rows // 5 // 8 * 8
    k = len(most)
    return [(k, 0, small), *((i, 0, part[0]) for i, part in enumerate(most)), (k, small, rows - 2 * small), (k, rows - small, small)]


def kernel(n, count, *refs):
    g, w, m_in, v_in = (refs[i : i + 3] for i in range(0, 12, 3))
    layers, chips = g[0].shape[0], n // 2
    new = [refs[12 + k * layers : 12 + (k + 1) * layers] for k in range(3)]
    refs = refs[12 + 3 * layers :]
    m, v, own, held = (refs[i : i + 3] for i in range(0, 12, 3))
    (squares, own_sem, pair_send, pair_recv, ring_send, ring_recv, hand_send, norm_send, norm_recv, state_sem, held_sem) = refs[12:]
    pieces = [(k, l, first, rows) for k, first, rows in cuts([one.shape[1:] for one in held]) for l in range(layers)]
    blocks = [(k, l) for k in range(3) for l in range(layers)]
    me = lax.axis_index("dp")
    h, z = lax.rem(me, 2), lax.div(me, 2)
    partner = me + 1 - 2 * h
    up, down = lax.rem(me + 2, n), lax.rem(me + n - 2, n)
    onward = [up, down]

    def remote(src, dst, send, recv, device):
        return pltpu.make_async_remote_copy(
            src_ref=src, dst_ref=dst, send_sem=send, recv_sem=recv, device_id={"dp": device}, device_id_type=MESH
        )

    def chunk(l, stage):
        return lax.rem(z + 2 * chips - 1 - stage, chips) if l == 0 else lax.rem(z + 1 + stage, chips)

    def own_copy(i, stage):
        k, l, first, rows = pieces[i]
        c, at = chunk(l, stage), pl.ds(first, rows)
        return pltpu.make_async_copy(g[k].at[l, 2 * c + h, at], own[k].at[l, c, at], own_sem.at[i])

    def held_copy(k, l):
        return pltpu.make_async_copy(g[k].at[l, 2 * chunk(l, 0) + 1 - h], held[k].at[l], held_sem.at[k, l])

    def pair_copy(i, stage, start=False):
        k, l, first, rows = pieces[i]
        c, at = chunk(l, stage), pl.ds(first, rows)
        src = held[k].at[l, at] if start else g[k].at[l, 2 * c + 1 - h, at]
        return remote(src, new[k][l].at[2 * c + h, at], pair_send.at[i], pair_recv.at[stage, i], partner)

    def ring_copy(i, stage):
        k, l, first, rows = pieces[i]
        c, at = chunk(l, stage), pl.ds(first, rows)
        return remote(own[k].at[l, c, at], new[k][l].at[2 * c + h, at], ring_send.at[i], ring_recv.at[stage, i], onward[l])

    def gather_copy(i, c, step):
        k, l, first, rows = pieces[i]
        block = new[k][l].at[2 * c + h, pl.ds(first, rows)]
        return remote(block, block, ring_send.at[i], ring_recv.at[step, i], onward[l])

    def hand_copy(i, c, step):
        k, l, first, rows = pieces[i]
        block = new[k][l].at[2 * c + h, pl.ds(first, rows)]
        return remote(block, block, hand_send.at[i], pair_recv.at[step, i], partner)

    def state_copies(k, l):
        return [
            pltpu.make_async_copy(m_in[k].at[l], m[k].at[l], state_sem.at[0, k, l]),
            pltpu.make_async_copy(v_in[k].at[l], v[k].at[l], state_sem.at[1, k, l]),
            pltpu.make_async_copy(w[k].at[l, me], held[k].at[l], held_sem.at[k, l]),
        ]

    def add(i, stage, arrived, total=0, squared=False):
        k, l, first, rows = pieces[i]
        c = chunk(l, stage)
        columns = own[k].shape[-1]
        tile = row_tile(rows, columns)

        def body(j, total):
            at = pl.ds(pl.multiple_of(first + j * tile, 8), tile)
            x = own[k][l, c, at, :].astype(F32) + new[k][l][2 * c + 1 - h, at, :].astype(F32)
            if arrived:
                x = x + new[k][l][2 * c + h, at, :].astype(F32)
            x = x.astype(BF16)
            own[k][l, c, at, :] = x
            if not squared:
                return total
            y = x.astype(F32)
            y = y * y
            y = sum(y[:, j : j + 128] for j in range(0, columns, 128))
            return total + sum(y[j : j + 8] for j in range(0, tile, 8))

        return lax.fori_loop(0, rows // tile, body, total)

    everyone = range(len(pieces))

    for k, l in blocks:
        held_copy(k, l).start()
    for i in everyone:
        own_copy(i, 0).start()

    barrier = pltpu.get_barrier_semaphore()
    for other in (partner, up, down):
        pl.semaphore_signal(barrier, inc=1, device_id={"dp": other}, device_id_type=MESH)
    for k, l in blocks:
        held_copy(k, l).wait()
    pl.semaphore_wait(barrier, 3)

    for i in everyone:
        pair_copy(i, 0, True).start()
    for i in everyone:
        own_copy(i, 0).wait()
        pair_copy(i, 0).wait_recv()
        add(i, 0, False)
        ring_copy(i, 0).start()
    for i in everyone:
        pair_copy(i, 0).wait_send()
        own_copy(i, 1).start()
        pair_copy(i, 1).start()
    for k, l in blocks:
        for copy in state_copies(k, l):
            copy.start()

    def middle(stage, _):
        for i in everyone:
            own_copy(i, stage).wait()
            pair_copy(i, stage).wait_recv()
            ring_copy(i, stage - 1).wait_recv()
            add(i, stage, True)
            ring_copy(i, stage - 1).wait_send()
            ring_copy(i, stage).start()
            pair_copy(i, stage).wait_send()
            own_copy(i, stage + 1).start()
            pair_copy(i, stage + 1).start()
        return 0

    last = chips - 1
    lax.fori_loop(1, last, middle, 0)
    total = jnp.zeros((8, 128), F32)
    for i in everyone:
        own_copy(i, last).wait()
        pair_copy(i, last).wait_recv()
        ring_copy(i, last - 1).wait_recv()
        total = add(i, last, True, total, True)

    squares[me] = jnp.sum(total, axis=0, keepdims=True)
    far = sorted(range(1, n), key=lambda j: -min(j, n - j))
    tell = [remote(squares.at[me], squares.at[me], norm_send.at[j], norm_recv.at[j], lax.rem(me + j, n)) for j in far]
    for one in tell:
        one.start()
    for k, l in blocks:
        for copy in state_copies(k, l):
            copy.wait()
    for i in everyone:
        ring_copy(i, last - 1).wait_send()
        pair_copy(i, last).wait_send()
    for one in tell[::-1]:
        one.wait_recv()
    everything = jnp.sum(jnp.sum(squares[...], axis=0), axis=1, keepdims=True)
    factor = jnp.minimum(1.0, 0.5 * lax.rsqrt(everything / count + 1e-30))

    for i in everyone:
        k, l, first, rows = pieces[i]
        tile = row_tile(rows, held[k].shape[-1])

        def body(j, _):
            at = pl.ds(pl.multiple_of(first + j * tile, 8), tile)
            x = own[k][l, z, at, :].astype(F32) * factor
            m_new = 0.9 * m[k][l, at, :] + 0.1 * x
            v_new = 0.95 * v[k][l, at, :] + 0.05 * x * x
            old = held[k][l, at, :].astype(F32)
            m[k][l, at, :] = m_new
            v[k][l, at, :] = v_new
            new[k][l][me, at, :] = (old - 0.02 * (m_new * lax.rsqrt(v_new + 1e-8) + 0.1 * old)).astype(BF16)
            return 0

        lax.fori_loop(0, rows // tile, body, 0)
        gather_copy(i, z, 0).start()
        hand_copy(i, z, 0).start()

    def forward(step, _):
        for i in everyone:
            c = chunk(pieces[i][1], step)
            gather_copy(i, c, step).wait_recv()
            gather_copy(i, c, step).wait_send()
            gather_copy(i, c, step + 1).start()
            hand_copy(i, c, step).wait_send()
            hand_copy(i, c, step + 1).start()
        return 0

    lax.fori_loop(0, last - 1, forward, 0)
    for i in everyone:
        c = chunk(pieces[i][1], last - 1)
        gather_copy(i, c, last - 1).wait_recv()
        hand_copy(i, c, last - 1).wait_send()
        hand_copy(i, c, last).start()
    for i in everyone:
        gather_copy(i, z, last - 1).wait_send()
    for one in tell:
        one.wait_send()

    def handed(step, _):
        for i in everyone:
            hand_copy(i, z, step).wait_recv()
        return 0

    lax.fori_loop(0, chips, handed, 0)
    for i in everyone:
        hand_copy(i, z, last).wait_send()


def put_out(layers, *refs):
    new, moments = refs[: 3 * layers], refs[3 * layers : 3 * layers + 6]
    outs, sem = refs[3 * layers + 6 : -1], refs[-1]
    pairs = [(one, outs[i // layers].at[i % layers]) for i, one in enumerate(new)] + list(zip(moments, outs[3:]))
    copies = [pltpu.make_async_copy(one, out, sem.at[i]) for i, (one, out) in enumerate(pairs)]
    for copy in copies:
        copy.start()
    for copy in copies:
        copy.wait()


def solution(mesh):
    n = mesh.shape["dp"]

    def step(*arrays):
        terms, weights, m, v = (arrays[i : i + 3] for i in (0, 3, 6, 9))
        layers = m[0].shape[0]
        parts = [one.shape[1:] for one in m]
        count = float(n * layers * sum(math.prod(part) for part in parts))
        cut = lambda a, part: a.reshape(layers, n, *part)
        terms = [cut(t, part) for t, part in zip(terms, parts)]
        weights = [cut(t, part) for t, part in zip(weights, parts)]
        chips, pieces = n // 2, layers * len(cuts(parts))
        sem = pltpu.SemaphoreType.DMA
        outs = [pltpu.VMEM((n, *part), BF16) for part in parts for _ in range(layers)] + [pltpu.VMEM((layers, *part), F32) for part in parts] * 2
        grant = 24 * 1024 * 1024
        result = pl.pallas_call(
            functools.partial(kernel, n, count),
            out_shape=outs,
            in_specs=[pl.BlockSpec(memory_space=pltpu.HBM)] * 12,
            out_specs=[pl.BlockSpec(memory_space=pltpu.VMEM)] * len(outs),
            scratch_shapes=[pltpu.VMEM((layers, chips, *part), BF16) for part in parts]
            + [pltpu.VMEM((layers, *part), BF16) for part in parts]
            + [
                pltpu.VMEM((n, 1, 128), F32),
                sem((pieces,)),
                sem((pieces,)),
                sem((chips, pieces)),
                sem((pieces,)),
                sem((chips - 1, pieces)),
                sem((pieces,)),
                sem((n,)),
                sem((n,)),
                sem((2, 3, layers)),
                sem((3, layers)),
            ],
            compiler_params=pltpu.CompilerParams(collective_id=0, has_side_effects=True, vmem_limit_bytes=grant),
        )(*(pltpu.with_memory_space_constraint(one, pltpu.HBM) for one in (*terms, *weights, *m, *v)))
        result = [pltpu.with_memory_space_constraint(one, pltpu.VMEM) for one in result]
        result = pl.pallas_call(
            functools.partial(put_out, layers),
            out_shape=[pltpu.HBM((layers, n, *part), BF16) for part in parts] + [pltpu.HBM((layers, *part), F32) for part in parts] * 2,
            in_specs=[pl.BlockSpec(memory_space=pltpu.VMEM)] * len(result),
            out_specs=[pl.BlockSpec(memory_space=pltpu.HBM)] * 9,
            scratch_shapes=[sem((len(result),))],
            compiler_params=pltpu.CompilerParams(vmem_limit_bytes=grant),
        )(*result)
        whole = [one.reshape(layers, -1, one.shape[-1]) for one in result[:3]]
        return (*whole, *result[3:])

    all_of, cut = P(None, None, None), P(None, "dp", None)
    return jax.shard_map(
        step,
        mesh=mesh,
        in_specs=(P(("rep", "dp"), None, None, None),) * 3 + (all_of,) * 3 + (cut,) * 6,
        out_specs=(P("rep", None, None),) * 3 + (P("rep", "dp", None),) * 6,
        check_vma=False,
    )
```

```python
import functools
import math

import jax
import jax.numpy as jnp
from jax import lax
from jax.experimental import pallas as pl
from jax.experimental.pallas import tpu as pltpu
from jax.sharding import PartitionSpec as P

MESH = pl.DeviceIdType.MESH
F32, BF16 = jnp.float32, jnp.bfloat16


def row_tile(rows, columns):
    best = 8
    for tile in range(8, rows + 1, 8):
        if rows % tile == 0 and tile * columns <= 32 * 1024:
            best = tile
    return best


def cuts(parts):
    *most, (rows, _) = parts
    small = rows // 5 // 8 * 8
    k = len(most)
    return [(k, 0, small), *((i, 0, part[0]) for i, part in enumerate(most)), (k, small, rows - 2 * small), (k, rows - small, small)]


def kernel(n, count, *refs):
    g, w, m_in, v_in = (refs[i : i + 3] for i in range(0, 12, 3))
    layers, chips = g[0].shape[0], n // 2
    new = [refs[12 + k * layers : 12 + (k + 1) * layers] for k in range(3)]
    refs = refs[12 + 3 * layers :]
    m, v, own, held = (refs[i : i + 3] for i in range(0, 12, 3))
    (squares, own_sem, held_sem, pair_send, pair_recv, ring_send, ring_recv, hand_send, hand_recv, norm_send, norm_recv) = refs[12:]
    pieces = [(k, l, first, rows) for k, first, rows in cuts([one.shape[1:] for one in held]) for l in range(layers)]
    weights = range(3)
    me = lax.axis_index("dp")
    h, z = lax.rem(me, 2), lax.div(me, 2)
    partner = me + 1 - 2 * h
    up, down = lax.rem(me + 2, n), lax.rem(me + n - 2, n)
    onward = [up, down]

    def remote(src, dst, send, recv, device):
        return pltpu.make_async_remote_copy(
            src_ref=src, dst_ref=dst, send_sem=send, recv_sem=recv, device_id={"dp": device}, device_id_type=MESH
        )

    def chunk(l, stage):
        return lax.rem(z + 2 * chips - 1 - stage, chips) if l == 0 else lax.rem(z + 1 + stage, chips)

    def own_copy(i, stage):
        k, l, first, rows = pieces[i]
        c, at = chunk(l, stage), pl.ds(first, rows)
        return pltpu.make_async_copy(g[k].at[l, 2 * c + h, at], own[k].at[l, c, at], own_sem.at[i])

    def held_copy(i):
        k, l, first, rows = pieces[i]
        at = pl.ds(first, rows)
        return pltpu.make_async_copy(g[k].at[l, 2 * chunk(l, 0) + 1 - h, at], held[k].at[l, at], held_sem.at[i])

    def pair_copy(i, stage, start=False):
        k, l, first, rows = pieces[i]
        c, at = chunk(l, stage), pl.ds(first, rows)
        src = held[k].at[l, at] if start else g[k].at[l, 2 * c + 1 - h, at]
        return remote(src, new[k][l].at[2 * c + h, at], pair_send.at[k], pair_recv.at[lax.rem(stage, 2), i], partner)

    def ring_copy(i, stage):
        k, l, first, rows = pieces[i]
        c, at = chunk(l, stage), pl.ds(first, rows)
        return remote(own[k].at[l, c, at], new[k][l].at[2 * c + h, at], ring_send.at[k], ring_recv.at[stage, i], onward[l])

    def gather_copy(i, c, step):
        k, l, first, rows = pieces[i]
        block = new[k][l].at[2 * c + h, pl.ds(first, rows)]
        return remote(block, block, ring_send.at[k], ring_recv.at[step, i], onward[l])

    def hand_copy(i, c):
        k, l, first, rows = pieces[i]
        block = new[k][l].at[2 * c + h, pl.ds(first, rows)]
        return remote(block, block, hand_send.at[k], hand_recv.at[k], partner)

    def state_copies(k):
        return [
            pltpu.make_async_copy(m_in[k], m[k], held_sem.at[k]),
            pltpu.make_async_copy(v_in[k], v[k], held_sem.at[3 + k]),
            pltpu.make_async_copy(w[k].at[:, me], held[k], held_sem.at[6 + k]),
        ]

    def all_of(k, stages, send, recv):
        block = own[k].at[:, pl.ds(0, stages)]
        return remote(block, block, send.at[k], recv.at[k], partner)

    def add(i, stage, arrived, total=0, squared=False):
        k, l, first, rows = pieces[i]
        c = chunk(l, stage)
        columns = own[k].shape[-1]
        tile = row_tile(rows, columns)

        def body(j, total):
            at = pl.ds(pl.multiple_of(first + j * tile, 8), tile)
            x = own[k][l, c, at, :].astype(F32) + new[k][l][2 * c + 1 - h, at, :].astype(F32)
            if arrived:
                x = x + new[k][l][2 * c + h, at, :].astype(F32)
            x = x.astype(BF16)
            own[k][l, c, at, :] = x
            if not squared:
                return total
            y = x.astype(F32)
            y = y * y
            y = sum(y[:, j : j + 128] for j in range(0, columns, 128))
            return total + sum(y[j : j + 8] for j in range(0, tile, 8))

        return lax.fori_loop(0, rows // tile, body, total)

    everyone = range(len(pieces))

    for i in everyone:
        held_copy(i).start()
        own_copy(i, 0).start()

    barrier = pltpu.get_barrier_semaphore()
    for other in (partner, up, down):
        pl.semaphore_signal(barrier, inc=1, device_id={"dp": other}, device_id_type=MESH)
    pl.semaphore_wait(barrier, 3)

    for i in everyone:
        held_copy(i).wait()
        pair_copy(i, 0, True).start()
    for i in everyone:
        own_copy(i, 0).wait()
        pair_copy(i, 0).wait_recv()
        add(i, 0, False)
        ring_copy(i, 0).start()
    for k in weights:
        all_of(k, 1, pair_send, hand_recv).wait_send()
    for i in everyone:
        own_copy(i, 1).start()
        pair_copy(i, 1).start()
    for k in weights:
        for copy in state_copies(k):
            copy.start()

    def middle(stage, _):
        for i in everyone:
            own_copy(i, stage).wait()
            pair_copy(i, stage).wait_recv()
            ring_copy(i, stage - 1).wait_recv()
            add(i, stage, True)
            ring_copy(i, stage).start()
            own_copy(i, stage + 1).start()
            pair_copy(i, stage + 1).start()
        return 0

    last = chips - 1
    lax.fori_loop(1, last, middle, 0)
    total = jnp.zeros((8, 128), F32)
    for i in everyone:
        own_copy(i, last).wait()
        pair_copy(i, last).wait_recv()
        ring_copy(i, last - 1).wait_recv()
        total = add(i, last, True, total, True)

    squares[me] = jnp.sum(total, axis=0, keepdims=True)
    far = sorted(range(1, n), key=lambda j: -min(j, n - j))
    for j in far:
        remote(squares.at[me], squares.at[me], norm_send, norm_recv, lax.rem(me + j, n)).start()
    for k in weights:
        for copy in state_copies(k):
            copy.wait()
        all_of(k, last, ring_send, hand_recv).wait_send()
        all_of(k, last, pair_send, hand_recv).wait_send()
    others = squares.at[pl.ds(0, n - 1)]
    remote(others, others, norm_send, norm_recv, partner).wait_recv()
    everything = jnp.sum(jnp.sum(squares[...], axis=0), axis=1, keepdims=True)
    factor = jnp.minimum(1.0, 0.5 * lax.rsqrt(everything / count + 1e-30))

    for i in everyone:
        k, l, first, rows = pieces[i]
        tile = row_tile(rows, held[k].shape[-1])

        def body(j, _):
            at = pl.ds(pl.multiple_of(first + j * tile, 8), tile)
            x = own[k][l, z, at, :].astype(F32) * factor
            m_new = 0.9 * m[k][l, at, :] + 0.1 * x
            v_new = 0.95 * v[k][l, at, :] + 0.05 * x * x
            old = held[k][l, at, :].astype(F32)
            m[k][l, at, :] = m_new
            v[k][l, at, :] = v_new
            new[k][l][me, at, :] = (old - 0.02 * (m_new * lax.rsqrt(v_new + 1e-8) + 0.1 * old)).astype(BF16)
            return 0

        lax.fori_loop(0, rows // tile, body, 0)
        gather_copy(i, z, 0).start()
        hand_copy(i, z).start()

    def forward(step, _):
        for i in everyone:
            c = chunk(pieces[i][1], step)
            gather_copy(i, c, step).wait_recv()
            gather_copy(i, c, step + 1).start()
            hand_copy(i, c).start()
        return 0

    lax.fori_loop(0, last - 1, forward, 0)
    for i in everyone:
        c = chunk(pieces[i][1], last - 1)
        gather_copy(i, c, last - 1).wait_recv()
        hand_copy(i, c).start()
    remote(others, others, norm_send, norm_recv, partner).wait_send()
    for k in weights:
        all_of(k, last, ring_send, hand_recv).wait_send()
    for k in weights:
        all_of(k, chips, hand_send, hand_recv).wait()


def put_out(layers, *refs):
    new, moments = refs[: 3 * layers], refs[3 * layers : 3 * layers + 6]
    outs, sem = refs[3 * layers + 6 : -1], refs[-1]
    pairs = [(one, outs[i // layers].at[i % layers]) for i, one in enumerate(new)] + list(zip(moments, outs[3:]))
    copies = [pltpu.make_async_copy(one, out, sem.at[i]) for i, (one, out) in enumerate(pairs)]
    for copy in copies:
        copy.start()
    for copy in copies:
        copy.wait()


def solution(mesh):
    n = mesh.shape["dp"]

    def step(*arrays):
        terms, weights, m, v = (arrays[i : i + 3] for i in (0, 3, 6, 9))
        layers = m[0].shape[0]
        parts = [one.shape[1:] for one in m]
        count = float(n * layers * sum(math.prod(part) for part in parts))
        cut = lambda a, part: a.reshape(layers, n, *part)
        terms = [cut(t, part) for t, part in zip(terms, parts)]
        weights = [cut(t, part) for t, part in zip(weights, parts)]
        chips, pieces = n // 2, layers * len(cuts(parts))
        sem = pltpu.SemaphoreType.DMA
        outs = [pltpu.VMEM((n, *part), BF16) for part in parts for _ in range(layers)] + [pltpu.VMEM((layers, *part), F32) for part in parts] * 2
        grant = 24 * 1024 * 1024
        result = pl.pallas_call(
            functools.partial(kernel, n, count),
            out_shape=outs,
            in_specs=[pl.BlockSpec(memory_space=pltpu.HBM)] * 12,
            out_specs=[pl.BlockSpec(memory_space=pltpu.VMEM)] * len(outs),
            scratch_shapes=[pltpu.VMEM((layers, chips, *part), BF16) for part in parts]
            + [pltpu.VMEM((layers, *part), BF16) for part in parts]
            + [
                pltpu.VMEM((n, 1, 128), F32),
                sem((pieces,)),
                sem((pieces,)),
                sem((3,)),
                sem((2, pieces)),
                sem((3,)),
                sem((chips - 1, pieces)),
                sem((3,)),
                sem((3,)),
                sem,
                sem,
            ],
            compiler_params=pltpu.CompilerParams(collective_id=0, has_side_effects=True, vmem_limit_bytes=grant),
        )(*(pltpu.with_memory_space_constraint(one, pltpu.HBM) for one in (*terms, *weights, *m, *v)))
        result = [pltpu.with_memory_space_constraint(one, pltpu.VMEM) for one in result]
        result = pl.pallas_call(
            functools.partial(put_out, layers),
            out_shape=[pltpu.HBM((layers, n, *part), BF16) for part in parts] + [pltpu.HBM((layers, *part), F32) for part in parts] * 2,
            in_specs=[pl.BlockSpec(memory_space=pltpu.VMEM)] * len(result),
            out_specs=[pl.BlockSpec(memory_space=pltpu.HBM)] * 9,
            scratch_shapes=[sem((len(result),))],
            compiler_params=pltpu.CompilerParams(vmem_limit_bytes=grant),
        )(*result)
        whole = [one.reshape(layers, -1, one.shape[-1]) for one in result[:3]]
        return (*whole, *result[3:])

    all_of, cut = P(None, None, None), P(None, "dp", None)
    return jax.shard_map(
        step,
        mesh=mesh,
        in_specs=(P(("rep", "dp"), None, None, None),) * 3 + (all_of,) * 3 + (cut,) * 6,
        out_specs=(P("rep", None, None),) * 3 + (P("rep", "dp", None),) * 6,
        check_vma=False,
    )
```

```python
import functools
import math

import jax
import jax.numpy as jnp
from jax import lax
from jax.experimental import pallas as pl
from jax.experimental.pallas import tpu as pltpu
from jax.sharding import PartitionSpec as P


MESH = pl.DeviceIdType.MESH
F32, BF16 = jnp.float32, jnp.bfloat16


def row_tile(rows, columns):
    best = 8
    for tile in range(8, rows + 1, 8):
        if rows % tile == 0 and tile * columns <= 32 * 1024:
            best = tile
    return best


def cuts(parts):
    *most, (rows, _) = parts
    small = rows // 5 // 8 * 8
    k = len(most)
    return [(k, 0, small), *((i, 0, part[0]) for i, part in enumerate(most)), (k, small, rows - 2 * small), (k, rows - small, small)]


def kernel(n, count, *refs):
    g, w, m_in, v_in = (refs[i : i + 3] for i in range(0, 12, 3))
    layers, chips = g[0].shape[0], n // 2
    by_layer = lambda refs: [refs[k * layers : (k + 1) * layers] for k in range(3)]
    fresh, refs = by_layer(refs[12:]), refs[12 + 3 * layers :]
    m, v, own, held = (refs[i : i + 3] for i in range(0, 12, 3))
    new, refs = by_layer(refs[12:]), refs[12 + 3 * layers :]
    (squares, own_sem, held_sem, pair_send, pair_recv, ring_send, ring_recv, norm_send, norm_recv) = refs
    pieces = [(k, l, first, rows) for k, first, rows in cuts([one.shape[1:] for one in held]) for l in range(layers)]
    weights = range(3)
    me = lax.axis_index("dp")
    h, z = lax.rem(me, 2), lax.div(me, 2)
    partner = me + 1 - 2 * h
    up, down = lax.rem(me + 2, n), lax.rem(me + n - 2, n)
    onward = [up, down]

    def remote(src, dst, send, recv, device):
        return pltpu.make_async_remote_copy(
            src_ref=src, dst_ref=dst, send_sem=send, recv_sem=recv, device_id={"dp": device}, device_id_type=MESH
        )

    def chunk(l, stage):
        return lax.rem(z + 2 * chips - 1 - stage, chips) if l == 0 else lax.rem(z + 1 + stage, chips)

    def own_copy(i, stage):
        k, l, first, rows = pieces[i]
        c, at = chunk(l, stage), pl.ds(first, rows)
        return pltpu.make_async_copy(g[k].at[l, 2 * c + h, at], own[k].at[l, c, at], own_sem.at[i])

    def held_copy(i):
        k, l, first, rows = pieces[i]
        at = pl.ds(first, rows)
        return pltpu.make_async_copy(g[k].at[l, 2 * chunk(l, 0) + 1 - h, at], held[k].at[l, at], held_sem.at[i])

    def pair_copy(i, stage, start=False):
        k, l, first, rows = pieces[i]
        c, at = chunk(l, stage), pl.ds(first, rows)
        src = held[k].at[l, at] if start else g[k].at[l, 2 * c + 1 - h, at]
        return remote(src, new[k][l].at[2 * c + h, at], pair_send.at[k], pair_recv.at[lax.rem(stage, 2), i], partner)

    def ring_copy(i, stage):
        k, l, first, rows = pieces[i]
        c, at = chunk(l, stage), pl.ds(first, rows)
        return remote(own[k].at[l, c, at], new[k][l].at[2 * c + h, at], ring_send.at[k], ring_recv.at[lax.rem(stage, 3), i], onward[l])

    def state_copies(k):
        return [
            pltpu.make_async_copy(m_in[k], m[k], held_sem.at[k]),
            pltpu.make_async_copy(v_in[k], v[k], held_sem.at[3 + k]),
            pltpu.make_async_copy(w[k].at[:, me], held[k], held_sem.at[6 + k]),
        ]

    def all_of(k, stages, send):
        block = own[k].at[:, pl.ds(0, stages)]
        return remote(block, block, send.at[k], send.at[k], partner)

    def add(i, stage, arrived, total=0, squared=False):
        k, l, first, rows = pieces[i]
        c = chunk(l, stage)
        columns = own[k].shape[-1]
        tile = row_tile(rows, columns)

        def body(j, total):
            at = pl.ds(pl.multiple_of(first + j * tile, 8), tile)
            x = own[k][l, c, at, :].astype(F32) + new[k][l][2 * c + 1 - h, at, :].astype(F32)
            if arrived:
                x = x + new[k][l][2 * c + h, at, :].astype(F32)
            x = x.astype(BF16)
            own[k][l, c, at, :] = x
            if not squared:
                return total
            y = x.astype(F32)
            y = y * y
            y = sum(y[:, j : j + 128] for j in range(0, columns, 128))
            return total + sum(y[j : j + 8] for j in range(0, tile, 8))

        return lax.fori_loop(0, rows // tile, body, total)

    everyone = range(len(pieces))

    for i in everyone:
        held_copy(i).start()
        own_copy(i, 0).start()

    barrier = pltpu.get_barrier_semaphore()
    for other in (partner, up, down):
        pl.semaphore_signal(barrier, inc=1, device_id={"dp": other}, device_id_type=MESH)
    pl.semaphore_wait(barrier, 3)

    for i in everyone:
        held_copy(i).wait()
        pair_copy(i, 0, True).start()
    for i in everyone:
        own_copy(i, 0).wait()
        pair_copy(i, 0).wait_recv()
        add(i, 0, False)
        ring_copy(i, 0).start()
    for k in weights:
        all_of(k, 1, pair_send).wait_send()
    for i in everyone:
        own_copy(i, 1).start()
        pair_copy(i, 1).start()
    for k in weights:
        for copy in state_copies(k):
            copy.start()

    def middle(stage, _):
        for i in everyone:
            own_copy(i, stage).wait()
            pair_copy(i, stage).wait_recv()
            ring_copy(i, stage - 1).wait_recv()
            add(i, stage, True)
            ring_copy(i, stage).start()
            own_copy(i, stage + 1).start()
            pair_copy(i, stage + 1).start()
        return 0

    last = chips - 1
    lax.fori_loop(1, last, middle, 0)
    total = jnp.zeros((8, 128), F32)
    for i in everyone:
        own_copy(i, last).wait()
        pair_copy(i, last).wait_recv()
        ring_copy(i, last - 1).wait_recv()
        total = add(i, last, True, total, True)

    squares[me] = jnp.sum(total, axis=0, keepdims=True)
    far = sorted(range(1, n), key=lambda j: -min(j, n - j))
    for j in far:
        remote(squares.at[me], squares.at[me], norm_send, norm_recv, lax.rem(me + j, n)).start()
    for k in weights:
        for copy in state_copies(k):
            copy.wait()
        all_of(k, last, ring_send).wait_send()
        all_of(k, last, pair_send).wait_send()
    others = squares.at[pl.ds(0, n - 1)]
    remote(others, others, norm_send, norm_recv, partner).wait_recv()
    everything = jnp.sum(jnp.sum(squares[...], axis=0), axis=1, keepdims=True)
    factor = jnp.minimum(1.0, 0.5 * lax.rsqrt(everything / count + 1e-30))

    for i in everyone:
        k, l, first, rows = pieces[i]
        tile = row_tile(rows, held[k].shape[-1])

        def body(j, _):
            at = pl.ds(pl.multiple_of(first + j * tile, 8), tile)
            x = own[k][l, z, at, :].astype(F32) * factor
            m_new = 0.9 * m[k][l, at, :] + 0.1 * x
            v_new = 0.95 * v[k][l, at, :] + 0.05 * x * x
            old = held[k][l, at, :].astype(F32)
            m[k][l, at, :] = m_new
            v[k][l, at, :] = v_new
            fresh[k][l][at, :] = (old - 0.02 * (m_new * lax.rsqrt(v_new + 1e-8) + 0.1 * old)).astype(BF16)
            return 0

        lax.fori_loop(0, rows // tile, body, 0)
    remote(others, others, norm_send, norm_recv, partner).wait_send()


def put_out(*refs):
    half = len(refs) // 2
    copies = [pltpu.make_async_copy(refs[i], refs[half + i], refs[-1].at[i]) for i in range(half)]
    for copy in copies:
        copy.start()
    for copy in copies:
        copy.wait()


def place(n, step, layers, *refs):
    blocks, out, sem = refs[: 2 * layers], refs[-2], refs[-1]
    chips = n // 2
    me = lax.axis_index("dp")
    h, z = lax.rem(me, 2), lax.div(me, 2)
    copies = []
    for i, block in enumerate(blocks):
        l = i % layers
        c = lax.rem(z + chips - step, chips) if l == 0 else lax.rem(z + step, chips)
        row = 2 * c + (h if i < layers else 1 - h)
        copies.append(pltpu.make_async_copy(block, out.at[l, row], sem.at[i]))
    for copy in copies:
        copy.start()
    for copy in copies:
        copy.wait()


def solution(mesh):
    n = mesh.shape["dp"]

    def step(*arrays):
        terms, weights, m, v = (arrays[i : i + 3] for i in (0, 3, 6, 9))
        layers = m[0].shape[0]
        parts = [one.shape[1:] for one in m]
        count = float(n * layers * sum(math.prod(part) for part in parts))
        cut = lambda a, part: a.reshape(layers, n, *part)
        terms = [cut(t, part) for t, part in zip(terms, parts)]
        weights = [cut(t, part) for t, part in zip(weights, parts)]
        chips, pieces = n // 2, layers * len(cuts(parts))
        sem = pltpu.SemaphoreType.DMA
        vmem, hbm = pl.BlockSpec(memory_space=pltpu.VMEM), pl.BlockSpec(memory_space=pltpu.HBM)
        outs = [pltpu.VMEM(part, BF16) for part in parts for _ in range(layers)] + [pltpu.VMEM((layers, *part), F32) for part in parts] * 2
        grant = 44 * 1024 * 1024
        result = pl.pallas_call(
            functools.partial(kernel, n, count),
            out_shape=outs,
            in_specs=[hbm] * 12,
            out_specs=[vmem] * len(outs),
            scratch_shapes=[pltpu.VMEM((layers, chips, *part), BF16) for part in parts]
            + [pltpu.VMEM((layers, *part), BF16) for part in parts]
            + [pltpu.VMEM((n, *part), BF16) for part in parts for _ in range(layers)]
            + [
                pltpu.VMEM((n, 1, 128), F32),
                sem((pieces,)),
                sem((pieces,)),
                sem((3,)),
                sem((2, pieces)),
                sem((3,)),
                sem((3, pieces)),
                sem,
                sem,
            ],
            compiler_params=pltpu.CompilerParams(collective_id=0, has_side_effects=True, vmem_limit_bytes=grant),
        )(*(pltpu.with_memory_space_constraint(one, pltpu.HBM) for one in (*terms, *weights, *m, *v)))
        moments = result[3 * layers :]
        moments = pl.pallas_call(
            put_out,
            out_shape=[pltpu.HBM(one.shape, one.dtype) for one in moments],
            in_specs=[vmem] * len(moments),
            out_specs=[hbm] * len(moments),
            scratch_shapes=[sem((len(moments),))],
            cost_estimate=pl.CostEstimate(flops=0, bytes_accessed=sum(2 * 4 * one.size for one in moments), transcendentals=0),
            compiler_params=pltpu.CompilerParams(vmem_limit_bytes=grant),
        )(*(pltpu.with_memory_space_constraint(one, pltpu.VMEM) for one in moments))

        onward = [[(i, (i + 2) % n) for i in range(n)], [(i, (i - 2) % n) for i in range(n)]]
        other = [(i, i + 1 - 2 * (i % 2)) for i in range(n)]
        held = [result[k * layers : (k + 1) * layers] for k in range(3)]
        whole = [None] * 3
        for at in range(chips):
            for k in range(3):
                handed = [lax.ppermute(one, "dp", other) for one in held[k]]
                args = [*held[k], *handed] + ([whole[k]] if at else [])
                whole[k] = pl.pallas_call(
                    functools.partial(place, n, at, layers),
                    out_shape=pltpu.HBM((layers, n, *parts[k]), BF16),
                    in_specs=[vmem] * (2 * layers) + [hbm] * bool(at),
                    out_specs=hbm,
                    scratch_shapes=[sem((2 * layers,))],
                    input_output_aliases={2 * layers: 0} if at else {},
                    cost_estimate=pl.CostEstimate(flops=0, bytes_accessed=8 * layers * math.prod(parts[k]), transcendentals=0),
                    compiler_params=pltpu.CompilerParams(has_side_effects=True, vmem_limit_bytes=8 * 1024 * 1024),
                )(*args)
                if at + 1 < chips:
                    held[k] = [lax.ppermute(one, "dp", onward[l]) for l, one in enumerate(held[k])]
        whole = [one.reshape(layers, -1, one.shape[-1]) for one in whole]
        return (*whole, *moments)

    all_of, cut = P(None, None, None), P(None, "dp", None)
    return jax.shard_map(
        step,
        mesh=mesh,
        in_specs=(P(("rep", "dp"), None, None, None),) * 3 + (all_of,) * 3 + (cut,) * 6,
        out_specs=(P("rep", None, None),) * 3 + (P("rep", "dp", None),) * 6,
        check_vma=False,
    )
```

```python
import functools
import math

import jax
import jax.numpy as jnp
from jax import lax
from jax.experimental import pallas as pl
from jax.experimental.pallas import tpu as pltpu
from jax.sharding import PartitionSpec as P


MESH = pl.DeviceIdType.MESH
F32, BF16 = jnp.float32, jnp.bfloat16


def row_tile(rows, columns):
    best = 8
    for tile in range(8, rows + 1, 8):
        if rows % tile == 0 and tile * columns <= 32 * 1024:
            best = tile
    return best


def cuts(parts):
    *most, (rows, _) = parts
    small = rows // 5 // 8 * 8
    k = len(most)
    return [(k, 0, small), *((i, 0, part[0]) for i, part in enumerate(most)), (k, small, rows - 2 * small), (k, rows - small, small)]


def take_step(factor, g, w, m, v, w_new, m_new, v_new):
    rows, columns = g.shape
    tile = row_tile(rows, columns)

    def body(j, _):
        at = pl.ds(pl.multiple_of(j * tile, 8), tile)
        x = g[at, :].astype(F32) * factor
        one = 0.9 * m[at, :] + 0.1 * x
        two = 0.95 * v[at, :] + 0.05 * x * x
        old = w[at, :].astype(F32)
        m_new[at, :] = one
        v_new[at, :] = two
        w_new[at, :] = (old - 0.02 * (one * lax.rsqrt(two + 1e-8) + 0.1 * old)).astype(BF16)
        return 0

    lax.fori_loop(0, rows // tile, body, 0)


def later_step(layers, *refs):
    g, w, m, v, scale = refs[:5]
    w_new, (m_new, v_new) = refs[5 : 5 + layers], refs[5 + layers :]
    for l in range(layers):
        take_step(scale[:1, :1], g.at[l], w.at[l], m.at[l], v.at[l], w_new[l], m_new.at[l], v_new.at[l])


def kernel(n, count, *refs):
    g, w, m_in, v_in = (refs[i : i + 3] for i in range(0, 12, 3))
    layers, chips = g[0].shape[0], n // 2
    by_layer = lambda refs: [refs[k * layers : (k + 1) * layers] for k in range(3)]
    fresh, refs = refs[12 : 12 + layers], refs[12 + layers :]
    m, v = refs[:3], refs[3:6]
    sums, scale, own, held = (None, *refs[6:8]), refs[10], refs[11:14], (refs[14], *refs[8:10])
    new, refs = by_layer(refs[15:]), refs[15 + 3 * layers :]
    (squares, own_sem, held_sem, pair_send, pair_recv, ring_send, ring_recv, norm_send, norm_recv) = refs
    pieces = [(k, l, first, rows) for k, first, rows in cuts([one.shape[1:] for one in held]) for l in range(layers)]
    weights = range(3)
    me = lax.axis_index("dp")
    h, z = lax.rem(me, 2), lax.div(me, 2)
    partner = me + 1 - 2 * h
    up, down = lax.rem(me + 2, n), lax.rem(me + n - 2, n)
    onward = [up, down]

    def remote(src, dst, send, recv, device):
        return pltpu.make_async_remote_copy(
            src_ref=src, dst_ref=dst, send_sem=send, recv_sem=recv, device_id={"dp": device}, device_id_type=MESH
        )

    def chunk(l, stage):
        return lax.rem(z + 2 * chips - 1 - stage, chips) if l == 0 else lax.rem(z + 1 + stage, chips)

    def own_copy(i, stage):
        k, l, first, rows = pieces[i]
        c, at = chunk(l, stage), pl.ds(first, rows)
        return pltpu.make_async_copy(g[k].at[l, 2 * c + h, at], own[k].at[l, c, at], own_sem.at[i])

    def held_copy(i):
        k, l, first, rows = pieces[i]
        at = pl.ds(first, rows)
        return pltpu.make_async_copy(g[k].at[l, 2 * chunk(l, 0) + 1 - h, at], held[k].at[l, at], held_sem.at[i])

    def pair_copy(i, stage, start=False):
        k, l, first, rows = pieces[i]
        c, at = chunk(l, stage), pl.ds(first, rows)
        src = held[k].at[l, at] if start else g[k].at[l, 2 * c + 1 - h, at]
        return remote(src, new[k][l].at[2 * c + h, at], pair_send.at[k], pair_recv.at[lax.rem(stage, 2), i], partner)

    def ring_copy(i, stage):
        k, l, first, rows = pieces[i]
        c, at = chunk(l, stage), pl.ds(first, rows)
        return remote(own[k].at[l, c, at], new[k][l].at[2 * c + h, at], ring_send.at[k], ring_recv.at[lax.rem(stage, 3), i], onward[l])

    def state_copies(k):
        return [
            pltpu.make_async_copy(m_in[k], m[k], held_sem.at[k]),
            pltpu.make_async_copy(v_in[k], v[k], held_sem.at[3 + k]),
            pltpu.make_async_copy(w[k].at[:, me], held[k], held_sem.at[6 + k]),
        ]

    def all_of(k, stages, send):
        block = own[k].at[:, pl.ds(0, stages)]
        return remote(block, block, send.at[k], send.at[k], partner)

    def add(i, stage, arrived, total=0, squared=False):
        k, l, first, rows = pieces[i]
        c = chunk(l, stage)
        columns = own[k].shape[-1]
        tile = row_tile(rows, columns)

        def body(j, total):
            at = pl.ds(pl.multiple_of(first + j * tile, 8), tile)
            x = own[k][l, c, at, :].astype(F32) + new[k][l][2 * c + 1 - h, at, :].astype(F32)
            if arrived:
                x = x + new[k][l][2 * c + h, at, :].astype(F32)
            x = x.astype(BF16)
            if not squared:
                own[k][l, c, at, :] = x
                return total
            if k:
                sums[k][l, at, :] = x
            else:
                own[k][l, c, at, :] = x
            y = x.astype(F32)
            y = y * y
            y = sum(y[:, j : j + 128] for j in range(0, columns, 128))
            return total + sum(y[j : j + 8] for j in range(0, tile, 8))

        return lax.fori_loop(0, rows // tile, body, total)

    everyone = range(len(pieces))

    barrier = pltpu.get_barrier_semaphore()
    for other in (up, down, partner):
        pl.semaphore_signal(barrier, inc=1, device_id={"dp": other}, device_id_type=MESH)

    for i in everyone:
        held_copy(i).start()
        own_copy(i, 0).start()
    pl.semaphore_wait(barrier, 3)

    for i in everyone:
        held_copy(i).wait()
        pair_copy(i, 0, True).start()
    for i in everyone:
        own_copy(i, 0).wait()
        pair_copy(i, 0).wait_recv()
        add(i, 0, False)
        ring_copy(i, 0).start()
    for k in weights:
        all_of(k, 1, pair_send).wait_send()
    for i in everyone:
        own_copy(i, 1).start()
        pair_copy(i, 1).start()
    for k in weights:
        for copy in state_copies(k):
            copy.start()

    def middle(stage, _):
        for i in everyone:
            own_copy(i, stage).wait()
            pair_copy(i, stage).wait_recv()
            ring_copy(i, stage - 1).wait_recv()
            add(i, stage, True)
            ring_copy(i, stage).start()
            own_copy(i, stage + 1).start()
            pair_copy(i, stage + 1).start()
        return 0

    last = chips - 1
    lax.fori_loop(1, last, middle, 0)
    total = jnp.zeros((8, 128), F32)
    for i in everyone:
        own_copy(i, last).wait()
        pair_copy(i, last).wait_recv()
        ring_copy(i, last - 1).wait_recv()
        total = add(i, last, True, total, True)

    squares[me] = jnp.sum(total, axis=0, keepdims=True)
    far = sorted(range(1, n), key=lambda j: -min(j, n - j))
    for j in far:
        remote(squares.at[me], squares.at[me], norm_send, norm_recv, lax.rem(me + j, n)).start()
    for k in weights:
        for copy in state_copies(k):
            copy.wait()
        all_of(k, last, ring_send).wait_send()
        all_of(k, last, pair_send).wait_send()
    others = squares.at[pl.ds(0, n - 1)]
    remote(others, others, norm_send, norm_recv, partner).wait_recv()
    everything = jnp.sum(jnp.sum(squares[...], axis=0), axis=1, keepdims=True)
    factor = jnp.minimum(1.0, 0.5 * lax.rsqrt(everything / count + 1e-30))

    scale[...] = jnp.broadcast_to(factor, scale.shape)
    for l in range(layers):
        take_step(factor, own[0].at[l, z], held[0].at[l], m[0].at[l], v[0].at[l], fresh[l], m[0].at[l], v[0].at[l])
    remote(others, others, norm_send, norm_recv, partner).wait_send()


def put_out(*refs):
    half = len(refs) // 2
    copies = [pltpu.make_async_copy(refs[i], refs[half + i], refs[-1].at[i]) for i in range(half)]
    for copy in copies:
        copy.start()
    for copy in copies:
        copy.wait()


def place(n, step, layers, *refs):
    blocks, out, sem = refs[: 2 * layers], refs[-2], refs[-1]
    chips = n // 2
    me = lax.axis_index("dp")
    h, z = lax.rem(me, 2), lax.div(me, 2)
    copies = []
    for i, block in enumerate(blocks):
        l = i % layers
        c = lax.rem(z + chips - step, chips) if l == 0 else lax.rem(z + step, chips)
        row = 2 * c + (h if i < layers else 1 - h)
        copies.append(pltpu.make_async_copy(block, out.at[l, row], sem.at[i]))
    for copy in copies:
        copy.start()
    for copy in copies:
        copy.wait()


def solution(mesh):
    n = mesh.shape["dp"]

    def step(*arrays):
        terms, weights, m, v = (arrays[i : i + 3] for i in (0, 3, 6, 9))
        layers = m[0].shape[0]
        parts = [one.shape[1:] for one in m]
        count = float(n * layers * sum(math.prod(part) for part in parts))
        cut = lambda a, part: a.reshape(layers, n, *part)
        terms = [cut(t, part) for t, part in zip(terms, parts)]
        weights = [cut(t, part) for t, part in zip(weights, parts)]
        chips, pieces = n // 2, layers * len(cuts(parts))
        sem = pltpu.SemaphoreType.DMA
        vmem, hbm = pl.BlockSpec(memory_space=pltpu.VMEM), pl.BlockSpec(memory_space=pltpu.HBM)
        outs = [pltpu.VMEM(parts[0], BF16)] * layers + [pltpu.VMEM((layers, *part), F32) for part in parts] * 2
        outs += [pltpu.VMEM((layers, *part), BF16) for part in parts[1:]] * 2 + [pltpu.VMEM((8, 128), F32)]
        grant = 44 * 1024 * 1024
        result = pl.pallas_call(
            functools.partial(kernel, n, count),
            out_shape=outs,
            in_specs=[hbm] * 12,
            out_specs=[vmem] * len(outs),
            scratch_shapes=[pltpu.VMEM((layers, chips, *part), BF16) for part in parts]
            + [pltpu.VMEM((layers, *parts[0]), BF16)]
            + [pltpu.VMEM((n, *part), BF16) for part in parts for _ in range(layers)]
            + [
                pltpu.VMEM((n, 1, 128), F32),
                sem((pieces,)),
                sem((pieces,)),
                sem((3,)),
                sem((2, pieces)),
                sem((3,)),
                sem((3, pieces)),
                sem,
                sem,
            ],
            compiler_params=pltpu.CompilerParams(collective_id=0, has_side_effects=True, vmem_limit_bytes=grant),
        )(*(pltpu.with_memory_space_constraint(one, pltpu.HBM) for one in (*terms, *weights, *m, *v)))
        held, rest = [result[:layers]], result[layers:]
        m, v, sums, old, scale = list(rest[:3]), list(rest[3:6]), rest[6:8], rest[8:10], rest[10]
        in_vmem = lambda args: [pltpu.with_memory_space_constraint(one, pltpu.VMEM) for one in args]
        for k in (1, 2):
            state = pltpu.VMEM((layers, *parts[k]), F32)
            *one, m[k], v[k] = pl.pallas_call(
                functools.partial(later_step, layers),
                out_shape=[pltpu.VMEM(parts[k], BF16)] * layers + [state] * 2,
                in_specs=[vmem] * 5,
                out_specs=[vmem] * (layers + 2),
                cost_estimate=pl.CostEstimate(flops=0, bytes_accessed=22 * layers * math.prod(parts[k]), transcendentals=0),
                compiler_params=pltpu.CompilerParams(vmem_limit_bytes=grant),
            )(*in_vmem([sums[k - 1], old[k - 1], m[k], v[k], scale]))
            held.append(one)
        moments = [*m, *v]
        moments = pl.pallas_call(
            put_out,
            out_shape=[pltpu.HBM(one.shape, one.dtype) for one in moments],
            in_specs=[vmem] * len(moments),
            out_specs=[hbm] * len(moments),
            scratch_shapes=[sem((len(moments),))],
            cost_estimate=pl.CostEstimate(flops=0, bytes_accessed=sum(2 * 4 * one.size for one in moments), transcendentals=0),
            compiler_params=pltpu.CompilerParams(vmem_limit_bytes=grant),
        )(*in_vmem(moments))

        onward = [[(i, (i + 2) % n) for i in range(n)], [(i, (i - 2) % n) for i in range(n)]]
        other = [(i, i + 1 - 2 * (i % 2)) for i in range(n)]
        whole = [None] * 3
        for at in range(chips):
            for k in range(3):
                handed = [lax.ppermute(one, "dp", other) for one in held[k]]
                args = [*held[k], *handed] + ([whole[k]] if at else [])
                whole[k] = pl.pallas_call(
                    functools.partial(place, n, at, layers),
                    out_shape=pltpu.HBM((layers, n, *parts[k]), BF16),
                    in_specs=[vmem] * (2 * layers) + [hbm] * bool(at),
                    out_specs=hbm,
                    scratch_shapes=[sem((2 * layers,))],
                    input_output_aliases={2 * layers: 0} if at else {},
                    cost_estimate=pl.CostEstimate(flops=0, bytes_accessed=8 * layers * math.prod(parts[k]), transcendentals=0),
                    compiler_params=pltpu.CompilerParams(has_side_effects=True, vmem_limit_bytes=8 * 1024 * 1024),
                )(*args)
                if at + 1 < chips:
                    held[k] = [lax.ppermute(one, "dp", onward[l]) for l, one in enumerate(held[k])]
        whole = [one.reshape(layers, -1, one.shape[-1]) for one in whole]
        return (*whole, *moments)

    all_of, cut = P(None, None, None), P(None, "dp", None)
    return jax.shard_map(
        step,
        mesh=mesh,
        in_specs=(P(("rep", "dp"), None, None, None),) * 3 + (all_of,) * 3 + (cut,) * 6,
        out_specs=(P("rep", None, None),) * 3 + (P("rep", "dp", None),) * 6,
        check_vma=False,
    )
```
